32 devices in a mesh: seg: 16 (over z, x, core), freq: 2 (over y).
Axes of the slice: x: 2, y: 2, z: 4, core: 2. Of those that a mesh axis runs over, the one named last changes fastest.
Arguments:
- coarse: float32 [64, 128, 2048], P('seg', None, 'freq'), may hold values from 0.5 to 8
- offsets: int32 [64, 32], replicated, may hold values from -8 to 8, as said below
Outputs:
- fine: float32 [32, 128, 2048], P(None, 'seg', 'freq')
- peaks: float32 [128], P('seg')
The draws below stay inside these ranges and needn't reach their ends.
Inputs may be any that keep to these rules, and one draw needn't show every extreme that they name: `offsets`: every entry lies in -8 to 8, and both ends occur in every draw.
All inputs are finite; a program needn't handle non-finite values.
Results may differ from the reference program's by a relative error of at most 0.0003.
Values sent between devices are 32-bit elements; how exact they have to be, the bound alone decides.
A program may use at most 128 MiB of HBM per device.

```python
import math
import jax
import jax.numpy as jnp
from jax import lax

SPINDOWNS = 32
HALO = 8
SEGMENTS = 64
SKY_POINTS = 128
BINS = 2048


def draw_offsets(key, part):
    base = jax.random.randint(jax.random.fold_in(key, 11), (SEGMENTS, SPINDOWNS), -HALO, HALO + 1, dtype=jnp.int32)
    first_seg = jax.random.randint(jax.random.fold_in(key, 12), (), 0, SEGMENTS, dtype=jnp.int32)
    step_seg = jax.random.randint(jax.random.fold_in(key, 13), (), 1, SEGMENTS, dtype=jnp.int32)
    second_seg = (first_seg + step_seg) % SEGMENTS
    first_spin = jax.random.randint(jax.random.fold_in(key, 14), (), 0, SPINDOWNS, dtype=jnp.int32)
    second_spin = jax.random.randint(jax.random.fold_in(key, 15), (), 0, SPINDOWNS, dtype=jnp.int32)
    base = base.at[first_seg, first_spin].set(HALO)
    base = base.at[second_seg, second_spin].set(-HALO)
    return base


def shard_levels(stream_key, shape, pieces, smallest, largest):
    gain = 1.0
    for dim, parts in pieces:
        steps = jax.random.uniform(jax.random.fold_in(jax.random.fold_in(stream_key, 6), dim), (parts,), jnp.float32, smallest / len(pieces), largest / len(pieces))
        gain = gain * jnp.repeat(jnp.exp(steps), shape[dim] // parts).reshape((-1,) + (1,) * (len(shape) - 1 - dim))
    return gain


def setup_inputs(seed: int = 0) -> dict:
    streams_of = jax.random.split(jax.random.key(seed), 3)
    coarse = jnp.clip(jnp.exp(math.log(8.0) - 2.7725887 * jax.random.uniform(streams_of[0], (SEGMENTS, SKY_POINTS, BINS), jnp.float32) ** shard_levels(streams_of[0], (SEGMENTS, SKY_POINTS, BINS), ((0, 16), (2, 2)), -0.2, 0.2)), 0.5, 8.0)
    offsets = draw_offsets(jax.random.fold_in(streams_of[2], 71), 0)
    return {"coarse": coarse, "offsets": offsets}


def window(line, begin):
    return lax.dynamic_slice_in_dim(line, begin, line.shape[1] - 2 * HALO, 1)


def reference(coarse, offsets):
    padded = jnp.pad(coarse, ((0, 0), (0, 0), (HALO, HALO)))

    def spindown(column):
        starts = (HALO + column).astype(jnp.int32)
        shifted = jax.vmap(window)(padded, starts)
        return jnp.sum(shifted, axis=0) / SEGMENTS

    fine = lax.map(spindown, offsets.T)
    peaks = jnp.max(fine, axis=(0, 2))
    return fine, peaks
```

```python
import functools

import jax
import jax.numpy as jnp
from jax import lax
from jax.experimental import pallas as pl
from jax.experimental.pallas import tpu as pltpu
from jax.sharding import PartitionSpec as P

HALO = 8
EDGE = 128
SHIFTS = 2 * HALO + 1
MESH = pl.DeviceIdType.MESH


def partner(me, step, count):
    if count & (count - 1):
        return lax.rem(step + count - me, count)
    result = me
    bit = 1
    while bit < count:
        wanted = lax.rem(step // bit, 2)
        held = lax.rem(me // bit, 2)
        result = result + bit * wanted * (1 - 2 * held)
        bit *= 2
    return result


def kernel(
    nseg,
    nfreq,
    coarse,
    offsets,
    total,
    peaks,
    maps,
    low,
    high,
    shifted,
    tops,
    own_sem,
    send_sem,
    recv_sem,
    up_send,
    up_recv,
    down_send,
    down_recv,
    top_send,
    top_recv,
):
    local_segs = coarse.shape[0]
    spins, rows, bins = total.shape
    me = lax.axis_index("seg")
    band = lax.axis_index("freq")

    def mine(target):
        return coarse.at[:, pl.ds(pl.multiple_of(target * rows, rows), rows), :]

    def exchange(step):
        other = partner(me, step, nseg)
        return pltpu.make_async_remote_copy(
            src_ref=mine(other),
            dst_ref=maps.at[step],
            send_sem=send_sem.at[step],
            recv_sem=recv_sem.at[step],
            device_id={"seg": other, "freq": band},
            device_id_type=MESH,
        )

    def upward(step):
        return pltpu.make_async_remote_copy(
            src_ref=maps.at[step, :, :, pl.ds(bins - EDGE, EDGE)],
            dst_ref=low.at[step],
            send_sem=up_send.at[step],
            recv_sem=up_recv.at[step],
            device_id={"seg": me, "freq": band + 1},
            device_id_type=MESH,
        )

    def downward(step):
        return pltpu.make_async_remote_copy(
            src_ref=maps.at[step, :, :, pl.ds(0, EDGE)],
            dst_ref=high.at[step],
            send_sem=down_send.at[step],
            recv_sem=down_recv.at[step],
            device_id={"seg": me, "freq": band - 1},
            device_id_type=MESH,
        )

    own = pltpu.make_async_copy(mine(me), maps.at[0], own_sem)
    own.start()

    barrier = pltpu.get_barrier_semaphore()

    @pl.loop(1, nseg)
    def _(step):
        pl.semaphore_signal(
            barrier, inc=1, device_id={"seg": partner(me, step, nseg), "freq": band}, device_id_type=MESH
        )

    for step in range(1, nfreq):
        pl.semaphore_signal(
            barrier, inc=1, device_id={"seg": me, "freq": lax.rem(band + step, nfreq)}, device_id_type=MESH
        )

    total[...] = jnp.zeros_like(total)

    @pl.when(band == 0)
    def _():
        low[...] = jnp.zeros_like(low)

    @pl.when(band == nfreq - 1)
    def _():
        high[...] = jnp.zeros_like(high)

    pl.semaphore_wait(barrier, nseg - 1 + nfreq - 1)

    @pl.loop(1, nseg)
    def _(step):
        exchange(step).start()

    def forward(step):
        @pl.when(band < nfreq - 1)
        def _():
            upward(step).start()

        @pl.when(band > 0)
        def _():
            downward(step).start()

    def add(step):
        @pl.when(band < nfreq - 1)
        def _():
            downward(step).wait_recv()

        @pl.when(band > 0)
        def _():
            upward(step).wait_recv()

        first = partner(me, step, nseg) * local_segs
        lane = lax.broadcasted_iota(jnp.int32, (rows, EDGE), 1)
        for seg in range(local_segs):
            ring = jnp.where(lane < EDGE // 2, high[step, seg], low[step, seg])
            line = jnp.concatenate([maps[step, seg], ring], axis=1)
            width = bins + EDGE
            for shift in range(-HALO, HALO + 1):
                turned = line if shift == 0 else pltpu.roll(line, (-shift) % width, 1)
                shifted[seg, HALO + shift] = turned[:, :bins]

        def spindown(spin, carry):
            value = total[spin]
            for seg in range(local_segs):
                value = value + shifted[seg, HALO + offsets[spin, first + seg]]
            total[spin] = value
            return carry

        lax.fori_loop(0, spins, spindown, 0, unroll=2)

    own.wait()
    forward(0)

    @pl.loop(1, nseg)
    def _(step):
        exchange(step).wait_recv()
        forward(step)
        add(step - 1)

    add(nseg - 1)

    best = total[0]
    for spin in range(1, spins):
        best = jnp.maximum(best, total[spin])
    top = jnp.max(best, axis=1, keepdims=True) * (1.0 / (nseg * local_segs))
    tops[0] = jnp.broadcast_to(top, (rows, EDGE))

    def tell(step):
        return pltpu.make_async_remote_copy(
            src_ref=tops.at[0],
            dst_ref=tops.at[step],
            send_sem=top_send.at[step],
            recv_sem=top_recv.at[step],
            device_id={"seg": me, "freq": lax.rem(band + step, nfreq)},
            device_id_type=MESH,
        )

    for step in range(1, nfreq):
        tell(step).start()

    @pl.loop(1, nseg)
    def _(step):
        exchange(step).wait_send()

    @pl.loop(0, nseg)
    def _(step):
        @pl.when(band < nfreq - 1)
        def _():
            upward(step).wait_send()

        @pl.when(band > 0)
        def _():
            downward(step).wait_send()

    for step in range(1, nfreq):
        tell(step).wait()
    peak = tops[0]
    for step in range(1, nfreq):
        peak = jnp.maximum(peak, tops[step])
    peaks[...] = peak


def solution(mesh):
    nseg, nfreq = mesh.shape["seg"], mesh.shape["freq"]

    def on_device(coarse, offsets):
        local_segs, points, bins = coarse.shape
        rows = points // nseg
        spins = offsets.shape[1]
        total, peaks = pl.pallas_call(
            functools.partial(kernel, nseg, nfreq),
            out_shape=(
                jax.ShapeDtypeStruct((spins, rows, bins), jnp.float32),
                jax.ShapeDtypeStruct((rows, EDGE), jnp.float32),
            ),
            in_specs=[
                pl.BlockSpec(memory_space=pl.ANY),
                pl.BlockSpec(memory_space=pltpu.SMEM),
            ],
            out_specs=(
                pl.BlockSpec(memory_space=pltpu.VMEM),
                pl.BlockSpec(memory_space=pltpu.VMEM),
            ),
            scratch_shapes=[
                pltpu.VMEM((nseg, local_segs, rows, bins), jnp.float32),
                pltpu.VMEM((nseg, local_segs, rows, EDGE), jnp.float32),
                pltpu.VMEM((nseg, local_segs, rows, EDGE), jnp.float32),
                pltpu.VMEM((local_segs, SHIFTS, rows, bins), jnp.float32),
                pltpu.VMEM((nfreq, rows, EDGE), jnp.float32),
                pltpu.SemaphoreType.DMA,
                pltpu.SemaphoreType.DMA((nseg,)),
                pltpu.SemaphoreType.DMA((nseg,)),
                pltpu.SemaphoreType.DMA((nseg,)),
                pltpu.SemaphoreType.DMA((nseg,)),
                pltpu.SemaphoreType.DMA((nseg,)),
                pltpu.SemaphoreType.DMA((nseg,)),
                pltpu.SemaphoreType.DMA((nfreq,)),
                pltpu.SemaphoreType.DMA((nfreq,)),
            ],
            compiler_params=pltpu.CompilerParams(collective_id=0, has_side_effects=True),
        )(coarse, offsets.T)
        return total * (1.0 / (nseg * local_segs)), peaks[:, 0]

    return jax.shard_map(
        on_device,
        mesh=mesh,
        in_specs=(P("seg", None, "freq"), P()),
        out_specs=(P(None, "seg", "freq"), P("seg")),
        check_vma=False,
    )
```

```python
import functools

import jax
import jax.numpy as jnp
from jax import lax
from jax.experimental import pallas as pl
from jax.experimental.pallas import tpu as pltpu
from jax.sharding import PartitionSpec as P

HALO = 8
EDGE = 128
SHIFTS = 2 * HALO + 1
MESH = pl.DeviceIdType.MESH


def partner(me, step, count):
    if count & (count - 1):
        return lax.rem(step + count - me, count)
    result = me
    bit = 1
    while bit < count:
        wanted = lax.rem(step // bit, 2)
        held = lax.rem(me // bit, 2)
        result = result + bit * wanted * (1 - 2 * held)
        bit *= 2
    return result


def kernel(
    nseg,
    nfreq,
    coarse,
    offsets,
    total,
    peaks,
    maps,
    low,
    high,
    shifted,
    tops,
    shifts,
    own_sem,
    shifts_sem,
    edge_sem,
    edge_recv,
    send_sem,
    recv_sem,
    up_send,
    up_recv,
    down_send,
    down_recv,
    top_send,
    top_recv,
):
    local_segs = coarse.shape[0]
    spins, rows, bins = total.shape
    me = lax.axis_index("seg")
    band = lax.axis_index("freq")

    def mine(target):
        return coarse.at[:, pl.ds(pl.multiple_of(target * rows, rows), rows), :]

    early = EDGE if nfreq == 2 else bins
    edge_at = jnp.where(band == 0, bins - early, 0)
    rest_at = jnp.where(band == 0, 0, early)

    def piece(step, begin, size, sent, received):
        other = partner(me, step, nseg)
        columns = pl.ds(pl.multiple_of(begin, EDGE), size)
        rows_of = pl.ds(pl.multiple_of(other * rows, rows), rows)
        return pltpu.make_async_remote_copy(
            src_ref=coarse.at[:, rows_of, columns],
            dst_ref=maps.at[step, :, :, columns],
            send_sem=sent.at[step],
            recv_sem=received.at[step],
            device_id={"seg": other, "freq": band},
            device_id_type=MESH,
        )

    def edge(step):
        return piece(step, edge_at, early, edge_sem, edge_recv)

    def rest(step):
        return piece(step, rest_at, bins - early, send_sem, recv_sem)

    def upward(step):
        return pltpu.make_async_remote_copy(
            src_ref=maps.at[step, :, :, pl.ds(bins - EDGE, EDGE)],
            dst_ref=low.at[step],
            send_sem=up_send.at[step],
            recv_sem=up_recv.at[step],
            device_id={"seg": me, "freq": band + 1},
            device_id_type=MESH,
        )

    def downward(step):
        return pltpu.make_async_remote_copy(
            src_ref=maps.at[step, :, :, pl.ds(0, EDGE)],
            dst_ref=high.at[step],
            send_sem=down_send.at[step],
            recv_sem=down_recv.at[step],
            device_id={"seg": me, "freq": band - 1},
            device_id_type=MESH,
        )

    own = pltpu.make_async_copy(mine(me), maps.at[0], own_sem)
    own.start()

    barrier = pltpu.get_barrier_semaphore()

    @pl.loop(1, nseg)
    def _(step):
        pl.semaphore_signal(
            barrier, inc=1, device_id={"seg": partner(me, step, nseg), "freq": band}, device_id_type=MESH
        )

    for step in range(1, nfreq):
        pl.semaphore_signal(
            barrier, inc=1, device_id={"seg": me, "freq": lax.rem(band + step, nfreq)}, device_id_type=MESH
        )

    load_shifts = pltpu.make_async_copy(offsets, shifts, shifts_sem)
    load_shifts.start()
    total[...] = jnp.zeros_like(total)

    @pl.when(band == 0)
    def _():
        low[...] = jnp.zeros_like(low)

    @pl.when(band == nfreq - 1)
    def _():
        high[...] = jnp.zeros_like(high)

    pl.semaphore_wait(barrier, nseg - 1 + nfreq - 1)

    @pl.loop(1, nseg)
    def _(step):
        edge(step).start()

    if early < bins:

        @pl.loop(1, nseg)
        def _(step):
            rest(step).start()

    def forward(step):
        @pl.when(band < nfreq - 1)
        def _():
            upward(step).start()

        @pl.when(band > 0)
        def _():
            downward(step).start()

    def add(step):
        @pl.when(band < nfreq - 1)
        def _():
            downward(step).wait_recv()

        @pl.when(band > 0)
        def _():
            upward(step).wait_recv()

        first = partner(me, step, nseg) * local_segs
        lane = lax.broadcasted_iota(jnp.int32, (rows, EDGE), 1)
        for seg in range(local_segs):
            ring = jnp.where(lane < EDGE // 2, high[step, seg], low[step, seg])
            line = jnp.concatenate([maps[step, seg], ring], axis=1)
            width = bins + EDGE
            for shift in range(-HALO, HALO + 1):
                turned = line if shift == 0 else pltpu.roll(line, (-shift) % width, 1)
                shifted[seg, HALO + shift] = turned[:, :bins]

        def spindown(spin, carry):
            value = total[spin]
            for seg in range(local_segs):
                value = value + shifted[seg, HALO + shifts[spin, first + seg]]
            total[spin] = value
            return carry

        lax.fori_loop(0, spins, spindown, 0, unroll=2)

    own.wait()
    forward(0)

    @pl.loop(1, nseg)
    def _(step):
        edge(step).wait_recv()
        forward(step)

    load_shifts.wait()
    add(0)

    @pl.loop(1, nseg)
    def _(step):
        if early < bins:
            rest(step).wait_recv()
        add(step)

    best = total[0]
    for spin in range(1, spins):
        best = jnp.maximum(best, total[spin])
    top = jnp.max(best, axis=1, keepdims=True) * (1.0 / (nseg * local_segs))
    tops[0] = jnp.broadcast_to(top, (rows, EDGE))

    def tell(step):
        return pltpu.make_async_remote_copy(
            src_ref=tops.at[0],
            dst_ref=tops.at[step],
            send_sem=top_send.at[step],
            recv_sem=top_recv.at[step],
            device_id={"seg": me, "freq": lax.rem(band + step, nfreq)},
            device_id_type=MESH,
        )

    for step in range(1, nfreq):
        tell(step).start()

    @pl.loop(1, nseg)
    def _(step):
        edge(step).wait_send()
        if early < bins:
            rest(step).wait_send()

    @pl.loop(0, nseg)
    def _(step):
        @pl.when(band < nfreq - 1)
        def _():
            upward(step).wait_send()

        @pl.when(band > 0)
        def _():
            downward(step).wait_send()

    for step in range(1, nfreq):
        tell(step).wait()
    peak = tops[0]
    for step in range(1, nfreq):
        peak = jnp.maximum(peak, tops[step])
    peaks[...] = peak


def solution(mesh):
    nseg, nfreq = mesh.shape["seg"], mesh.shape["freq"]

    def on_device(coarse, offsets):
        local_segs, points, bins = coarse.shape
        rows = points // nseg
        spins = offsets.shape[1]
        total, peaks = pl.pallas_call(
            functools.partial(kernel, nseg, nfreq),
            out_shape=(
                jax.ShapeDtypeStruct((spins, rows, bins), jnp.float32),
                jax.ShapeDtypeStruct((rows, EDGE), jnp.float32),
            ),
            in_specs=[
                pl.BlockSpec(memory_space=pltpu.HBM),
                pl.BlockSpec(memory_space=pltpu.HBM),
            ],
            out_specs=(
                pl.BlockSpec(memory_space=pltpu.VMEM),
                pl.BlockSpec(memory_space=pltpu.VMEM),
            ),
            scratch_shapes=[
                pltpu.VMEM((nseg, local_segs, rows, bins), jnp.float32),
                pltpu.VMEM((nseg, local_segs, rows, EDGE), jnp.float32),
                pltpu.VMEM((nseg, local_segs, rows, EDGE), jnp.float32),
                pltpu.VMEM((local_segs, SHIFTS, rows, bins), jnp.float32),
                pltpu.VMEM((nfreq, rows, EDGE), jnp.float32),
                pltpu.SMEM(offsets.shape[::-1], jnp.int32),
                pltpu.SemaphoreType.DMA,
                pltpu.SemaphoreType.DMA,
                pltpu.SemaphoreType.DMA((nseg,)),
                pltpu.SemaphoreType.DMA((nseg,)),
                pltpu.SemaphoreType.DMA((nseg,)),
                pltpu.SemaphoreType.DMA((nseg,)),
                pltpu.SemaphoreType.DMA((nseg,)),
                pltpu.SemaphoreType.DMA((nseg,)),
                pltpu.SemaphoreType.DMA((nseg,)),
                pltpu.SemaphoreType.DMA((nseg,)),
                pltpu.SemaphoreType.DMA((nfreq,)),
                pltpu.SemaphoreType.DMA((nfreq,)),
            ],
            compiler_params=pltpu.CompilerParams(
                collective_id=0, has_side_effects=True, vmem_limit_bytes=32 << 20
            ),
        )(pltpu.with_memory_space_constraint(coarse, pltpu.HBM), pltpu.with_memory_space_constraint(offsets.T, pltpu.HBM))
        return total * (1.0 / (nseg * local_segs)), peaks[:, 0]

    return jax.shard_map(
        on_device,
        mesh=mesh,
        in_specs=(P("seg", None, "freq"), P()),
        out_specs=(P(None, "seg", "freq"), P("seg")),
        check_vma=False,
    )
```

```python
import functools

import jax
import jax.numpy as jnp
from jax import lax
from jax.experimental import pallas as pl
from jax.experimental.pallas import tpu as pltpu
from jax.sharding import PartitionSpec as P

HALO = 8
EDGE = 128
SHIFTS = 2 * HALO + 1
MESH = pl.DeviceIdType.MESH


def partner(me, step, count):
    if count & (count - 1):
        return lax.rem(step + count - me, count)
    result = me
    bit = 1
    while bit < count:
        wanted = (step // bit) % 2 if isinstance(step, int) else lax.rem(step // bit, 2)
        held = lax.rem(me // bit, 2)
        result = result + bit * wanted * (1 - 2 * held)
        bit *= 2
    return result


def kernel(
    nseg,
    nfreq,
    coarse,
    offsets,
    total,
    peaks,
    maps,
    low,
    high,
    shifted,
    tops,
    shifts,
    own_sem,
    shifts_sem,
    edge_sem,
    edge_recv,
    send_sem,
    recv_sem,
    up_send,
    up_recv,
    down_send,
    down_recv,
    top_send,
    top_recv,
):
    local_segs = coarse.shape[0]
    spins, rows, bins = total.shape
    parts = recv_sem.shape[0]
    part_segs = local_segs // parts
    scale = 1.0 / (nseg * local_segs)
    me = lax.axis_index("seg")
    band = lax.axis_index("freq")

    def mine(target):
        return coarse.at[:, pl.ds(pl.multiple_of(target * rows, rows), rows), :]

    early = EDGE if nfreq == 2 else bins
    edge_at = jnp.where(band == 0, bins - early, 0)
    rest_at = jnp.where(band == 0, 0, early)

    def piece(step, begin, size, segs, sent, received):
        other = partner(me, step, nseg)
        columns = pl.ds(pl.multiple_of(begin, EDGE), size)
        rows_of = pl.ds(pl.multiple_of(other * rows, rows), rows)
        return pltpu.make_async_remote_copy(
            src_ref=coarse.at[segs, rows_of, columns],
            dst_ref=maps.at[step, segs, :, columns],
            send_sem=sent,
            recv_sem=received,
            device_id={"seg": other, "freq": band},
            device_id_type=MESH,
        )

    def edge(step):
        return piece(step, edge_at, early, pl.ds(0, local_segs), edge_sem.at[step], edge_recv.at[step])

    def rest(step, part):
        segs = pl.ds(part * part_segs, part_segs)
        return piece(step, rest_at, bins - early, segs, send_sem.at[part, step], recv_sem.at[part, step])

    def upward(step):
        return pltpu.make_async_remote_copy(
            src_ref=maps.at[step, :, :, pl.ds(bins - EDGE, EDGE)],
            dst_ref=low.at[step],
            send_sem=up_send.at[step],
            recv_sem=up_recv.at[step],
            device_id={"seg": me, "freq": band + 1},
            device_id_type=MESH,
        )

    def downward(step):
        return pltpu.make_async_remote_copy(
            src_ref=maps.at[step, :, :, pl.ds(0, EDGE)],
            dst_ref=high.at[step],
            send_sem=down_send.at[step],
            recv_sem=down_recv.at[step],
            device_id={"seg": me, "freq": band - 1},
            device_id_type=MESH,
        )

    own = pltpu.make_async_copy(mine(me), maps.at[0], own_sem)
    own.start()

    barrier = pltpu.get_barrier_semaphore()

    for step in reversed(range(1, nseg)):
        pl.semaphore_signal(
            barrier, inc=1, device_id={"seg": partner(me, step, nseg), "freq": band}, device_id_type=MESH
        )

    for step in range(1, nfreq):
        pl.semaphore_signal(
            barrier, inc=1, device_id={"seg": me, "freq": lax.rem(band + step, nfreq)}, device_id_type=MESH
        )

    load_shifts = pltpu.make_async_copy(offsets, shifts, shifts_sem)
    load_shifts.start()
    total[...] = jnp.zeros_like(total)

    @pl.when(band == 0)
    def _():
        low[...] = jnp.zeros_like(low)

    @pl.when(band == nfreq - 1)
    def _():
        high[...] = jnp.zeros_like(high)

    pl.semaphore_wait(barrier, nseg - 1 + nfreq - 1)

    @pl.loop(1, nseg)
    def _(step):
        edge(step).start()

    if early < bins:

        @pl.loop(1, nseg)
        def _(step):
            for part in range(parts):
                rest(step, part).start()

    def forward(step):
        @pl.when(band < nfreq - 1)
        def _():
            upward(step).start()

        @pl.when(band > 0)
        def _():
            downward(step).start()

    def wait_edges(step):
        @pl.when(band < nfreq - 1)
        def _():
            downward(step).wait_recv()

        @pl.when(band > 0)
        def _():
            upward(step).wait_recv()

    def add(step, part, best=None):
        first = partner(me, step, nseg) * local_segs
        segs = range(part * part_segs, (part + 1) * part_segs)
        lane = lax.broadcasted_iota(jnp.int32, (rows, EDGE), 1)
        for seg in segs:
            ring = jnp.where(lane < EDGE // 2, high[step, seg], low[step, seg])
            line = jnp.concatenate([maps[step, seg], ring], axis=1)
            width = bins + EDGE
            for shift in range(-HALO, HALO + 1):
                turned = line if shift == 0 else pltpu.roll(line, (-shift) % width, 1)
                shifted[seg, HALO + shift] = turned[:, :bins]

        def spindown(spin, best):
            value = total[spin]
            for seg in segs:
                value = value + shifted[seg, HALO + shifts[spin, first + seg]]
            if best is not None:
                value = value * scale
                best = jnp.maximum(best, value)
            total[spin] = value
            return best

        return lax.fori_loop(0, spins, spindown, best, unroll=4)

    own.wait()
    forward(0)

    @pl.loop(1, nseg)
    def _(step):
        edge(step).wait_recv()
        forward(step)

    load_shifts.wait()
    wait_edges(0)
    for part in range(parts):
        add(0, part)

    def receive(step, best=None):
        wait_edges(step)
        for part in range(parts):
            if early < bins:
                rest(step, part).wait_recv()
            last = best if part == parts - 1 else None
            result = add(step, part, last)
        return result

    @pl.loop(1, nseg - 1)
    def _(step):
        receive(step)

    best = receive(nseg - 1, jnp.full((rows, bins), -jnp.inf, jnp.float32))
    top = best[:, :EDGE]
    for begin in range(EDGE, bins, EDGE):
        top = jnp.maximum(top, best[:, begin : begin + EDGE])
    tops[0] = top

    def tell(step):
        return pltpu.make_async_remote_copy(
            src_ref=tops.at[0],
            dst_ref=tops.at[step],
            send_sem=top_send.at[step],
            recv_sem=top_recv.at[step],
            device_id={"seg": me, "freq": lax.rem(band + step, nfreq)},
            device_id_type=MESH,
        )

    for step in range(1, nfreq):
        tell(step).start()

    @pl.loop(1, nseg)
    def _(step):
        edge(step).wait_send()
        if early < bins:
            for part in range(parts):
                rest(step, part).wait_send()

    @pl.loop(0, nseg)
    def _(step):
        @pl.when(band < nfreq - 1)
        def _():
            upward(step).wait_send()

        @pl.when(band > 0)
        def _():
            downward(step).wait_send()

    for step in range(1, nfreq):
        tell(step).wait()
    peak = tops[0]
    for step in range(1, nfreq):
        peak = jnp.maximum(peak, tops[step])
    peaks[...] = peak


def finish(total, tops, fine, peaks, sem):
    write = pltpu.make_async_copy(total, fine, sem)
    write.start()
    rows, width = tops.shape
    row = lax.broadcasted_iota(jnp.int32, (rows, width), 0)
    lane = lax.broadcasted_iota(jnp.int32, (rows, width), 1)
    top = jnp.max(tops[...], axis=1, keepdims=True)
    line = jnp.sum(jnp.where(row == lane, top, 0.0), axis=0)
    peaks[...] = line[:rows]
    write.wait()


def solution(mesh):
    nseg, nfreq = mesh.shape["seg"], mesh.shape["freq"]

    def on_device(coarse, offsets):
        local_segs, points, bins = coarse.shape
        rows = points // nseg
        spins = offsets.shape[1]
        parts = 1
        total, peaks = pl.pallas_call(
            functools.partial(kernel, nseg, nfreq),
            out_shape=(
                jax.ShapeDtypeStruct((spins, rows, bins), jnp.float32),
                jax.ShapeDtypeStruct((rows, EDGE), jnp.float32),
            ),
            in_specs=[
                pl.BlockSpec(memory_space=pltpu.HBM),
                pl.BlockSpec(memory_space=pltpu.HBM),
            ],
            out_specs=(
                pl.BlockSpec(memory_space=pltpu.VMEM),
                pl.BlockSpec(memory_space=pltpu.VMEM),
            ),
            scratch_shapes=[
                pltpu.VMEM((nseg, local_segs, rows, bins), jnp.float32),
                pltpu.VMEM((nseg, local_segs, rows, EDGE), jnp.float32),
                pltpu.VMEM((nseg, local_segs, rows, EDGE), jnp.float32),
                pltpu.VMEM((local_segs, SHIFTS, rows, bins), jnp.float32),
                pltpu.VMEM((nfreq, rows, EDGE), jnp.float32),
                pltpu.SMEM(offsets.shape[::-1], jnp.int32),
                pltpu.SemaphoreType.DMA,
                pltpu.SemaphoreType.DMA,
                pltpu.SemaphoreType.DMA((nseg,)),
                pltpu.SemaphoreType.DMA((nseg,)),
                pltpu.SemaphoreType.DMA((parts, nseg)),
                pltpu.SemaphoreType.DMA((parts, nseg)),
                pltpu.SemaphoreType.DMA((nseg,)),
                pltpu.SemaphoreType.DMA((nseg,)),
                pltpu.SemaphoreType.DMA((nseg,)),
                pltpu.SemaphoreType.DMA((nseg,)),
                pltpu.SemaphoreType.DMA((nfreq,)),
                pltpu.SemaphoreType.DMA((nfreq,)),
            ],
            compiler_params=pltpu.CompilerParams(
                collective_id=0, has_side_effects=True, vmem_limit_bytes=32 << 20
            ),
        )(pltpu.with_memory_space_constraint(coarse, pltpu.HBM), pltpu.with_memory_space_constraint(offsets.T, pltpu.HBM))
        return pl.pallas_call(
            finish,
            out_shape=(
                jax.ShapeDtypeStruct((spins, rows, bins), jnp.float32),
                jax.ShapeDtypeStruct((rows,), jnp.float32),
            ),
            in_specs=[pl.BlockSpec(memory_space=pltpu.VMEM), pl.BlockSpec(memory_space=pltpu.VMEM)],
            out_specs=(pl.BlockSpec(memory_space=pltpu.HBM), pl.BlockSpec(memory_space=pltpu.VMEM)),
            scratch_shapes=[pltpu.SemaphoreType.DMA],
            compiler_params=pltpu.CompilerParams(vmem_limit_bytes=8 << 20),
        )(total, peaks)

    return jax.shard_map(
        on_device,
        mesh=mesh,
        in_specs=(P("seg", None, "freq"), P()),
        out_specs=(P(None, "seg", "freq"), P("seg")),
        check_vma=False,
    )
```
